32 devices in a mesh: dp: 4 (over x, y), tp: 8 (over z, core).
Axes of the slice: x: 2, y: 2, z: 4, core: 2. Of those that a mesh axis runs over, the one named last changes fastest.
Arguments:
- x: bfloat16 [7168, 5120], P(('dp', 'tp')), parts along dimension 0
- dy: bfloat16 [7168, 5120], P(('dp', 'tp')), parts along dimension 0
- gate: bfloat16 [7168, 16384], P('dp', 'tp'), parts along dimension 0
- up: bfloat16 [7168, 16384], P('dp', 'tp'), parts along dimension 0
- w_gate: bfloat16 [5120, 16384], P(None, 'tp')
- w_up: bfloat16 [5120, 16384], P(None, 'tp')
- w_down: bfloat16 [16384, 5120], P('tp')
Outputs:
- output 1: bfloat16 [7168, 5120], P(('dp', 'tp')), parts along dimension 0
- output 2: bfloat16 [20480, 16384], P('dp', 'tp'), parts along dimension 0
- output 3: bfloat16 [20480, 16384], P('dp', 'tp'), parts along dimension 0
- output 4: bfloat16 [65536, 5120], P(('dp', 'tp')), parts along dimension 0
There are 4 independent parts. The reference program is written for one: setup_inputs(seed, part) draws one part's arguments, and reference() takes and returns one part's arrays. A program takes and returns all parts, laid end to end along the dimension named above; an argument that names none is the same for every part.
All inputs are finite; a program needn't handle non-finite values.
Results may differ from the reference program's by a relative error of at most 0.012.
Values are sent between devices in bfloat16 or wider.
A program may use at most 2 GiB of HBM per device.

```python
import jax
import jax.numpy as jnp

ROWS = 1792
D = 5120
FF = 16384


def act(gate, up):
    return jax.nn.silu(gate) * up


def setup_inputs(seed: int = 0, part: int = 0) -> dict:
    kx, ky, ka, kb, kg, ku, kd = jax.random.split(jax.random.key(seed), 7)
    kx, ky, ka, kb = (jax.random.fold_in(k, part) for k in (kx, ky, ka, kb))
    drawn = {
        "x": jax.random.normal(kx, (ROWS, D), jnp.float32),
        "dy": jax.random.normal(ky, (ROWS, D), jnp.float32),
        "gate": jax.random.normal(ka, (ROWS, FF), jnp.float32),
        "up": jax.random.normal(kb, (ROWS, FF), jnp.float32),
        "w_gate": jax.random.normal(kg, (D, FF), jnp.float32) * D**-0.5,
        "w_up": jax.random.normal(ku, (D, FF), jnp.float32) * D**-0.5,
        "w_down": jax.random.normal(kd, (FF, D), jnp.float32) * FF**-0.5,
    }
    return {k: v.astype(jnp.bfloat16) for k, v in drawn.items()}


def reference(x, dy, gate, up, w_gate, w_up, w_down):
    hidden, back = jax.vjp(act, gate.astype(jnp.float32), up.astype(jnp.float32))
    d_hidden = jnp.dot(dy, w_down.T, preferred_element_type=jnp.float32)
    d_gate, d_up = (g.astype(jnp.bfloat16) for g in back(d_hidden))
    dx = jnp.dot(d_gate, w_gate.T, preferred_element_type=jnp.float32) + jnp.dot(d_up, w_up.T, preferred_element_type=jnp.float32)
    dw_gate = jnp.dot(x.T, d_gate, preferred_element_type=jnp.float32)
    dw_up = jnp.dot(x.T, d_up, preferred_element_type=jnp.float32)
    dw_down = jnp.dot(hidden.astype(jnp.bfloat16).T, dy, preferred_element_type=jnp.float32)
    return tuple(g.astype(jnp.bfloat16) for g in (dx, dw_gate, dw_up, dw_down))
```

```python
import jax
import jax.numpy as jnp
from jax import lax
from jax.experimental import pallas as pl
from jax.experimental.pallas import tpu as pltpu
from jax.sharding import PartitionSpec as P

BF = jnp.bfloat16
F32 = jnp.float32
MESH = pl.DeviceIdType.MESH

R = 224
D = 5120
F = 2048
H = 2
HR = R // H
Q = 5
QC = D // Q
NH = 256
ND = 512
K2 = D // 2


def dot(a, b, ca, cb):
    return lax.dot_general(a, b, (((ca,), (cb,)), ((), ())), preferred_element_type=F32)


def kernel(
    x, dy, gate, up, w_gate, w_up, w_down,
    dx, dwg, dwu, dwd, dyg, xg, pown, psend, precv, rsend, rrecv,
    hid, dg, du, dyb, gub, wd, wgu, tile, ost, stf, stb, rsf,
    s_wd, s_wgu, s_gub, s_dyb, s_tile, s_out, s_st, s_rs,
    sd_r, sd_l, sd_p, rd, sx_r, sx_l, sx_p, rx, sp, rp, sr, rr,
):
    me = lax.axis_index("tp")
    z = me // 2
    c = lax.rem(me, 2)
    other = me + 1 - 2 * c
    right, left = me + 2, me - 2
    is_end = (z == 0) | (z == 3)
    is_mid = (z == 1) | (z == 2)
    zz = jnp.where(z < 2, z, 3 - z)

    def block_of(p):
        near = jnp.where((zz == 1) & (p < 2), 1 - p, p)
        return jnp.where(z < 2, near, 3 - near)

    def remote(src, dst, ssem, rsem, to):
        return pltpu.make_async_remote_copy(
            src_ref=src, dst_ref=dst, send_sem=ssem, recv_sem=rsem, device_id={"tp": to}, device_id_type=MESH
        )

    class Dy:
        own, all_, rs, ls, ps, rv, n = dy, dyg, sd_r, sd_l, sd_p, rd, H

        @staticmethod
        def own_at(i):
            return dy.at[pl.ds(i * HR, HR)]

        @staticmethod
        def at(blk, i):
            return dyg.at[blk, pl.ds(i * HR, HR)]

    class X:
        own, all_, rs, ls, ps, rv, n = x, xg, sx_r, sx_l, sx_p, rx, Q

        @staticmethod
        def own_at(i):
            return x.at[:, pl.ds(i * QC, QC)]

        @staticmethod
        def at(blk, i):
            return xg.at[blk, :, pl.ds(i * QC, QC)]

    def send_right(g, d, i, src):
        blk = me - 2 * d
        remote(src, g.at(blk, i), g.rs.at[d, i], g.rv.at[blk, i], right).start()

    def send_left(g, d, i, src):
        blk = me + 2 * d
        remote(src, g.at(blk, i), g.ls.at[d, i], g.rv.at[blk, i], left).start()

    def send_other(g, side, d, i, src):
        blk = me + (2 * d if side else -2 * d)
        remote(src, g.at(blk, i), g.ps.at[side, d, i], g.rv.at[blk, i], other).start()

    def wait_recv(g, blk, i):
        remote(g.at(blk, i), g.at(blk, i), g.ps.at[0, 0, i], g.rv.at[blk, i], other).wait_recv()

    def hop(g, d, i, gate_=True):
        @pl.when((z >= d) & gate_)
        def _():
            blk = me - 2 * d
            wait_recv(g, blk, i)

            @pl.when(z < 3)
            def _():
                send_right(g, d, i, g.at(blk, i))

            send_other(g, 0, d, i, g.at(blk, i))

        @pl.when((z + d <= 3) & gate_)
        def _():
            blk = me + 2 * d
            wait_recv(g, blk, i)

            @pl.when(z > 0)
            def _():
                send_left(g, d, i, g.at(blk, i))

            send_other(g, 1, d, i, g.at(blk, i))

    def wait_sends(g):
        def body(t, _):
            d, i = t // g.n, lax.rem(t, g.n)

            @pl.when((z < 3) & (d <= z))
            def _():
                remote(g.at(me, i), g.at(me, i), g.rs.at[d, i], g.rv.at[me, i], other).wait_send()

            @pl.when((z > 0) & (d <= 3 - z))
            def _():
                remote(g.at(me, i), g.at(me, i), g.ls.at[d, i], g.rv.at[me, i], other).wait_send()

            @pl.when(d <= z)
            def _():
                remote(g.at(me, i), g.at(me, i), g.ps.at[0, d, i], g.rv.at[me, i], other).wait_send()

            @pl.when((d > 0) & (d <= 3 - z))
            def _():
                remote(g.at(me, i), g.at(me, i), g.ps.at[1, d, i], g.rv.at[me, i], other).wait_send()

            return 0

        lax.fori_loop(0, 4 * g.n, body, 0)

    def x_step(s):
        @pl.when(s < Q)
        def _():
            send_other(X, 0, 0, s, X.own_at(s))

            @pl.when(is_mid)
            def _():
                send_right(X, 0, s, X.own_at(s))
                send_left(X, 0, s, X.own_at(s))

        @pl.when((s >= 1) & (s < Q + 1))
        def _():
            hop(X, 1, s - 1, is_mid)

        @pl.when((s >= 2) & (s < Q + 2))
        def _():
            hop(X, 2, s - 2, is_mid)

    def x_end(i):
        for d in (1, 2, 3):
            hop(X, d, i, is_end)

    def x_ready(i):
        for b in range(4):
            wait_recv(X, 2 * b + 1 - c, i)

    def wd_copy(n, slot):
        return pltpu.make_async_copy(w_down.at[pl.ds(n * NH, NH)], wd.at[slot], s_wd.at[slot])

    def wgu_copy(k, j, slot):
        src = w_up if k else w_gate
        return pltpu.make_async_copy(src.at[pl.ds(j * ND, ND)], wgu.at[slot, k], s_wgu.at[slot, k])

    def gub_copies(p):
        b = block_of(p)
        out = []
        for k, src in enumerate((gate, up)):
            for i, core in enumerate((c, 1 - c)):
                rows = pl.ds((2 * b + core) * R, R)
                out.append(pltpu.make_async_copy(src.at[rows], gub.at[k, pl.ds(i * R, R)], s_gub.at[k, i]))
        return out

    def dyb_copy(i, src):
        return pltpu.make_async_copy(src, dyb.at[pl.ds(i * R, R)], s_dyb.at[i])

    def tile_copies(own, all_, i, slot):
        cols = pl.ds(i * ND, ND)
        out = []
        for p in range(4):
            b = block_of(p)
            for k, core in enumerate((c, 1 - c)):
                src = own.at[:, cols] if p == 0 and k == 0 else all_.at[2 * b + core, :, cols]
                out.append(
                    pltpu.make_async_copy(src, tile.at[slot, pl.ds((2 * p + k) * R, R)], s_tile.at[slot, 2 * p + k])
                )
        return out

    def start(copies):
        for cp in copies:
            cp.start()

    def wait(copies):
        for cp in copies:
            cp.wait()

    def half(k):
        return pl.ds(pl.multiple_of(k * K2, K2), K2)

    def pair_send(p, k):
        return remote(psend.at[p, :, half(k)], precv.at[p, :, half(k)], sp.at[p, k], rp.at[p, k], other)

    def run_recv(t, k):
        return remote(rrecv.at[t, :, half(k)], rrecv.at[t, :, half(k)], sr.at[0, k], rr.at[t, k], other)

    def run_send(p, k, to, t):
        return remote(rsend.at[p, :, half(k)], rrecv.at[t, :, half(k)], sr.at[p, k], rr.at[t, k], to)

    def add_terms(p, k, extra, out):
        loads = [
            pltpu.make_async_copy(pown.at[p, :, half(k)], rsf, s_rs.at[0]),
            pltpu.make_async_copy(precv.at[p, :, half(k)], dyb.at[pl.ds(0, R), pl.ds(0, K2)], s_rs.at[1]),
        ]
        for n, t in enumerate(extra):
            loads.append(
                pltpu.make_async_copy(
                    rrecv.at[t, :, half(k)], dyb.at[pl.ds(R, R), pl.ds(n * K2, K2)], s_rs.at[2 + n]
                )
            )
        start(loads)
        wait(loads)

        def body(i, _):
            rows = pl.ds(pl.multiple_of(i * 32, 32), 32)
            low = pl.ds(pl.multiple_of(R + i * 32, 32), 32)
            v = rsf[rows] + dyb[rows, 0:K2].astype(F32)
            for n in range(len(extra)):
                v = v + dyb[low, n * K2 : (n + 1) * K2].astype(F32)
            dyb[rows, K2:D] = v.astype(BF)
            return 0

        lax.fori_loop(0, R // 32, body, 0)
        cp = pltpu.make_async_copy(dyb.at[pl.ds(0, R), pl.ds(K2, K2)], out, s_rs.at[4])
        cp.start()
        cp.wait()

    def pass_on(p, k, mid):
        t = block_of(p)
        pair_send(p, k).wait_recv()
        extra = ()
        if mid:
            run_recv(t, k).wait_recv()
            extra = (t,)
        add_terms(p, k, extra, rsend.at[p, :, half(k)])

        @pl.when(t > z)
        def _():
            run_send(p, k, right, t).start()

        @pl.when(t < z)
        def _():
            run_send(p, k, left, jnp.where(t == z - 1, 4, t)).start()

    def pass_on_both(p, mid):
        def body(k, _):
            pass_on(p, k, mid)
            return 0

        lax.fori_loop(0, 2, body, 0)

    barrier = pltpu.get_barrier_semaphore()

    def greet(to):
        pl.semaphore_signal(barrier, inc=1, device_id={"tp": to}, device_id_type=MESH)

    greet(other)

    @pl.when(z < 3)
    def _():
        greet(right)

    @pl.when(z > 0)
    def _():
        greet(left)

    for n in range(2):
        wd_copy(n, n).start()
    start(gub_copies(0))
    own_dyb = dyb_copy(0, dy)
    own_dyb.start()

    @pl.when(is_mid)
    def _():
        pl.semaphore_wait(barrier, 3)

    @pl.when(is_end)
    def _():
        pl.semaphore_wait(barrier, 2)

    for i in range(H):

        @pl.when(z < 3)
        def _():
            send_right(Dy, 0, i, Dy.own_at(i))

        @pl.when(z > 0)
        def _():
            send_left(Dy, 0, i, Dy.own_at(i))

        send_other(Dy, 0, 0, i, Dy.own_at(i))

    def end_x(i, _):
        @pl.when(z == 0)
        def _():
            send_right(X, 0, i, X.own_at(i))

        @pl.when(z == 3)
        def _():
            send_left(X, 0, i, X.own_at(i))

        return 0

    lax.fori_loop(0, Q, end_x, 0)
    for j in range(2):
        for k in range(2):
            wgu_copy(k, j, j).start()

    def phase(p, _):
        b = block_of(p)
        for i in range(H):
            wait_recv(Dy, 2 * b + 1 - c, i)
        theirs = dyb_copy(1, dyg.at[2 * b + 1 - c])
        theirs.start()

        @pl.when(p > 0)
        def _():
            dyb_copy(0, dyg.at[2 * b + c]).start()

        wait(gub_copies(p))
        own_dyb.wait()
        theirs.wait()
        rows = pl.ds(pl.multiple_of(p * 2 * R, 2 * R), 2 * R)

        def hidden_tile(n, _):
            slot = lax.rem(n, 2)
            cols = pl.ds(pl.multiple_of(n * NH, NH), NH)
            wd_copy(n, slot).wait()
            dh = dot(dyb[...], wd[slot], 1, 1)
            g = gub[0, :, cols].astype(F32)
            u = gub[1, :, cols].astype(F32)
            s = jax.nn.sigmoid(g)
            a = g * s
            hid[rows, cols] = (a * u).astype(BF)
            du[rows, cols] = (dh * a).astype(BF)
            dg[rows, cols] = (dh * (u * (s + a * (1.0 - s)))).astype(BF)

            @pl.when((n < F // NH - 2) | (p < 3))
            def _():
                wd_copy(lax.rem(n + 2, F // NH), slot).start()

            return 0

        lax.fori_loop(0, F // NH, hidden_tile, 0)

        @pl.when(p < 3)
        def _():
            start(gub_copies(p + 1))

        @pl.when(p < 3)
        def _():
            hop(Dy, p + 1, 0)

        @pl.when(p >= 2)
        def _():
            x_step(2 * p - 3)

            @pl.when(is_end)
            def _():
                pass_on_both(p - 1, False)

        def stage(j, slot):
            cols = pl.ds(pl.multiple_of(j * ND, ND), ND)
            return [
                pltpu.make_async_copy(stf.at[slot], pown.at[p, :, cols], s_st.at[0, slot]),
                pltpu.make_async_copy(stb.at[slot], psend.at[p, :, cols], s_st.at[1, slot]),
            ]

        def dx_tile(j, _):
            slot = lax.rem(j, 2)
            for k in range(2):
                wgu_copy(k, j, slot).wait()
            acc = dot(dg[rows, :], wgu[slot, 0], 1, 1) + dot(du[rows, :], wgu[slot, 1], 1, 1)

            @pl.when(j >= 2)
            def _():
                wait(stage(j - 2, slot))

            stf[slot] = acc[:R]
            stb[slot] = acc[R:].astype(BF)
            start(stage(j, slot))

            @pl.when((j < D // ND - 2) | (p < 3))
            def _():
                for k in range(2):
                    wgu_copy(k, lax.rem(j + 2, D // ND), slot).start()

            @pl.when(j == D // ND // 2 + 1)
            def _():
                pair_send(p, 0).start()

            return 0

        lax.fori_loop(0, D // ND, dx_tile, 0)
        for j in (D // ND - 2, D // ND - 1):
            wait(stage(j, j % 2))
        pair_send(p, 1).start()

        @pl.when(p < 3)
        def _():
            hop(Dy, p + 1, 1)

        @pl.when(p >= 1)
        def _():
            x_step(2 * p - 2)

        return 0

    lax.fori_loop(0, 4, phase, 0)

    def out_d(i, slot):
        cols = pl.ds(pl.multiple_of(i * ND, ND), ND)
        return pltpu.make_async_copy(ost.at[slot], dwd.at[:, cols], s_out.at[slot, 0])

    start(tile_copies(dy, dyg, 0, 0))

    def down_tile(i, _):
        slot = lax.rem(i, 2)

        @pl.when(i < D // ND - 1)
        def _():
            start(tile_copies(dy, dyg, i + 1, 1 - slot))

        @pl.when((i == 0) & is_end)
        def _():
            pass_on_both(3, False)

        @pl.when((i == 2) | (i == 4))
        def _():
            x_step(4 + i // 2)

        @pl.when(i == 7)
        def _():
            x_end(0)

        wait(tile_copies(dy, dyg, i, slot))

        @pl.when(i >= 2)
        def _():
            out_d(i - 2, slot).wait()

        for m in range(F // ND):
            ost[slot, m * ND : (m + 1) * ND, :] = dot(hid[:, m * ND : (m + 1) * ND], tile[slot], 0, 0).astype(BF)
        out_d(i, slot).start()
        return 0

    lax.fori_loop(0, D // ND, down_tile, 0)
    x_ready(0)
    start(tile_copies(x, xg, 0, 0))
    for i in (D // ND - 2, D // ND - 1):
        out_d(i, i % 2).wait()

    def out_gu(i, slot):
        rows = pl.ds(pl.multiple_of(i * ND, ND), ND)
        return [
            pltpu.make_async_copy(wgu.at[slot, k], (dwg, dwu)[k].at[rows], s_out.at[slot, k]) for k in range(2)
        ]

    def gu_tile(i, _):
        slot = lax.rem(i, 2)
        q = i // 2

        @pl.when((slot == 0) & (q < Q - 1))
        def _():
            x_end(q + 1)

        @pl.when((slot == 1) & (q < Q - 1))
        def _():
            x_ready(q + 1)

        @pl.when(i < D // ND - 1)
        def _():
            start(tile_copies(x, xg, i + 1, 1 - slot))

        @pl.when(is_mid & ((i == 2) | (i == 4)))
        def _():
            pass_on(3, i // 2 - 1, True)

        @pl.when(is_mid & (i == 5))
        def _():
            pass_on_both(2, True)

        @pl.when(is_mid & ((i == 6) | (i == 8)))
        def _():
            pass_on(1, i // 2 - 3, True)

        wait(tile_copies(x, xg, i, slot))

        @pl.when(i >= 2)
        def _():
            wait(out_gu(i - 2, slot))

        for k, r in enumerate((dg, du)):
            for n in range(2):
                wgu[slot, k, :, n * 1024 : (n + 1) * 1024] = dot(
                    tile[slot], r[:, n * 1024 : (n + 1) * 1024], 0, 0
                ).astype(BF)
        start(out_gu(i, slot))
        return 0

    lax.fori_loop(0, D // ND, gu_tile, 0)

    def last(k, _):
        pair_send(0, k).wait_recv()

        @pl.when(is_mid)
        def _():
            run_recv(z, k).wait_recv()
            run_recv(4, k).wait_recv()
            add_terms(0, k, (z, 4), dx.at[:, half(k)])

        @pl.when(is_end)
        def _():
            t = jnp.where(z == 0, 4, 3)
            run_recv(t, k).wait_recv()
            add_terms(0, k, (t,), dx.at[:, half(k)])

        return 0

    lax.fori_loop(0, 2, last, 0)
    for i in (D // ND - 2, D // ND - 1):
        wait(out_gu(i, i % 2))
    wait_sends(Dy)
    wait_sends(X)

    def sums(t, _):
        p, k = t // 2, lax.rem(t, 2)
        pair_send(p, k).wait_send()

        @pl.when(p > 0)
        def _():
            run_send(p, k, other, 0).wait_send()

        return 0

    lax.fori_loop(0, 8, sums, 0)


def fused(x, dy, gate, up, w_gate, w_up, w_down):
    hbm = pl.BlockSpec(memory_space=pl.ANY)

    def arr(*shape, dtype=BF):
        return jax.ShapeDtypeStruct(shape, dtype)

    outs = [
        arr(R, D), arr(D, F), arr(D, F), arr(F, D), arr(8, R, D), arr(8, R, D),
        arr(4, R, D, dtype=F32), arr(4, R, D), arr(4, R, D), arr(4, R, D), arr(5, R, D),
    ]
    dma = pltpu.SemaphoreType.DMA
    scratch = [
        pltpu.VMEM((8 * R, F), BF), pltpu.VMEM((8 * R, F), BF), pltpu.VMEM((8 * R, F), BF),
        pltpu.VMEM((2 * R, D), BF), pltpu.VMEM((2, 2 * R, F), BF), pltpu.VMEM((2, NH, D), BF),
        pltpu.VMEM((2, 2, ND, F), BF), pltpu.VMEM((2, 8 * R, ND), BF), pltpu.VMEM((2, F, ND), BF),
        pltpu.VMEM((2, R, ND), F32), pltpu.VMEM((2, R, ND), BF), pltpu.VMEM((R, K2), F32),
        dma((2,)), dma((2, 2)), dma((2, 2)), dma((2,)), dma((2, 8)), dma((2, 2)), dma((2, 2)), dma((5,)),
        dma((4, H)), dma((4, H)), dma((2, 4, H)), dma((8, H)),
        dma((4, Q)), dma((4, Q)), dma((2, 4, Q)), dma((8, Q)),
        dma((4, 2)), dma((4, 2)), dma((4, 2)), dma((5, 2)),
    ]
    return pl.pallas_call(
        kernel,
        out_shape=outs,
        in_specs=[hbm] * 7,
        out_specs=[hbm] * len(outs),
        scratch_shapes=scratch,
        compiler_params=pltpu.CompilerParams(
            collective_id=0, has_side_effects=True, vmem_limit_bytes=67043328
        ),
        cost_estimate=pl.CostEstimate(flops=225_000_000_000, bytes_accessed=500_000_000, transcendentals=4_000_000),
    )(x, dy, gate, up, w_gate, w_up, w_down)[:4]


def solution(mesh):
    rows, mine, cols = P(("dp", "tp"), None), P("dp", "tp"), P(None, "tp")
    return jax.shard_map(
        fused,
        mesh=mesh,
        in_specs=(rows, rows, mine, mine, cols, cols, P("tp", None)),
        out_specs=(rows, mine, mine, rows),
        check_vma=False,
    )
```

```python
import jax
import jax.numpy as jnp
from jax import lax
from jax.experimental import pallas as pl
from jax.experimental.pallas import tpu as pltpu
from jax.sharding import PartitionSpec as P

BF = jnp.bfloat16
F32 = jnp.float32
MESH = pl.DeviceIdType.MESH

R = 224
D = 5120
F = 2048
H = 2
HR = R // H
Q = 5
QC = D // Q
NH = 256
ND = 512
K2 = D // 2
NT = D // ND
NF = 4


def dot(a, b, ca, cb):
    return lax.dot_general(a, b, (((ca,), (cb,)), ((), ())), preferred_element_type=F32)


def order(z, p):
    zz = jnp.where(z < 2, z, 3 - z)
    near = jnp.where((zz == 1) & (p < 2), 1 - p, p)
    return jnp.where(z < 2, near, 3 - near)


def rows_copies(own, all_, i, dst, sems, block_of, c):
    cols = pl.ds(i * ND, ND)
    out = []
    for p in range(4):
        b = block_of(p)
        for k, core in enumerate((c, 1 - c)):
            src = own.at[:, cols] if p == 0 and k == 0 else all_.at[2 * b + core, :, cols]
            out.append(pltpu.make_async_copy(src, dst.at[pl.ds((2 * p + k) * R, R)], sems.at[2 * p + k]))
    return out


def kernel(
    x, dy, gate, up, w_gate, w_up, w_down,
    dxa, dwg, dwu, dwd, dgo, duo, xg, s_end, s_mid, dyg, pown, psend, precv, rsend, rrecv,
    hid, dg, du, dyb, gub, wd, wgu, tile, ost, stf, stb, rsf, rsb,
    s_wd, s_wgu, s_gub, s_dyb, s_tile, s_out, s_st, s_rs, s_keep,
    sd_r, sd_l, sd_p, rd, sx_r, sx_l, sx_p, rx, sp, rp, sr, rr,
):
    me = lax.axis_index("tp")
    z = me // 2
    c = lax.rem(me, 2)
    other = me + 1 - 2 * c
    right, left = me + 2, me - 2
    is_end = (z == 0) | (z == 3)
    is_mid = (z == 1) | (z == 2)

    def block_of(p):
        return order(z, p)

    def remote(src, dst, ssem, rsem, to):
        return pltpu.make_async_remote_copy(
            src_ref=src, dst_ref=dst, send_sem=ssem, recv_sem=rsem, device_id={"tp": to}, device_id_type=MESH
        )

    class Dy:
        own, all_, rs, ls, ps, rv, n = dy, dyg, sd_r, sd_l, sd_p, rd, H

        @staticmethod
        def own_at(i):
            return dy.at[pl.ds(i * HR, HR)]

        @staticmethod
        def at(blk, i):
            return dyg.at[blk, pl.ds(i * HR, HR)]

    class X:
        own, all_, rs, ls, ps, rv, n = x, xg, sx_r, sx_l, sx_p, rx, Q

        @staticmethod
        def own_at(i):
            return x.at[:, pl.ds(i * QC, QC)]

        @staticmethod
        def at(blk, i):
            return xg.at[blk, :, pl.ds(i * QC, QC)]

    def send_right(g, d, i, src):
        blk = me - 2 * d
        remote(src, g.at(blk, i), g.rs.at[d, i], g.rv.at[blk, i], right).start()

    def send_left(g, d, i, src):
        blk = me + 2 * d
        remote(src, g.at(blk, i), g.ls.at[d, i], g.rv.at[blk, i], left).start()

    def send_other(g, side, d, i, src):
        blk = me + (2 * d if side else -2 * d)
        remote(src, g.at(blk, i), g.ps.at[side, d, i], g.rv.at[blk, i], other).start()

    def wait_recv(g, blk, i):
        remote(g.at(blk, i), g.at(blk, i), g.ps.at[0, 0, i], g.rv.at[blk, i], other).wait_recv()

    def hop(g, d, i, gate_=True):
        @pl.when((z >= d) & gate_)
        def _():
            blk = me - 2 * d
            wait_recv(g, blk, i)

            @pl.when(z < 3)
            def _():
                send_right(g, d, i, g.at(blk, i))

            send_other(g, 0, d, i, g.at(blk, i))

        @pl.when((z + d <= 3) & gate_)
        def _():
            blk = me + 2 * d
            wait_recv(g, blk, i)

            @pl.when(z > 0)
            def _():
                send_left(g, d, i, g.at(blk, i))

            send_other(g, 1, d, i, g.at(blk, i))

    def wait_sends(g):
        def body(t, _):
            d, i = t // g.n, lax.rem(t, g.n)

            @pl.when((z < 3) & (d <= z))
            def _():
                remote(g.at(me, i), g.at(me, i), g.rs.at[d, i], g.rv.at[me, i], other).wait_send()

            @pl.when((z > 0) & (d <= 3 - z))
            def _():
                remote(g.at(me, i), g.at(me, i), g.ls.at[d, i], g.rv.at[me, i], other).wait_send()

            @pl.when(d <= z)
            def _():
                remote(g.at(me, i), g.at(me, i), g.ps.at[0, d, i], g.rv.at[me, i], other).wait_send()

            @pl.when((d > 0) & (d <= 3 - z))
            def _():
                remote(g.at(me, i), g.at(me, i), g.ps.at[1, d, i], g.rv.at[me, i], other).wait_send()

            return 0

        lax.fori_loop(0, 4 * g.n, body, 0)

    def x_step(s):
        @pl.when(s < Q)
        def _():
            send_other(X, 0, 0, s, X.own_at(s))

            @pl.when(is_mid)
            def _():
                send_right(X, 0, s, X.own_at(s))
                send_left(X, 0, s, X.own_at(s))

        @pl.when((s >= 1) & (s < Q + 1))
        def _():
            hop(X, 1, s - 1, is_mid)

        @pl.when((s >= 2) & (s < Q + 2))
        def _():
            hop(X, 2, s - 2, is_mid)

    def x_end(i):
        for d in (1, 2, 3):
            hop(X, d, i, is_end)

    def x_ready(i):
        for b in range(4):
            wait_recv(X, 2 * b + 1 - c, i)

    def wd_copy(n, slot):
        return pltpu.make_async_copy(w_down.at[pl.ds(n * NH, NH)], wd.at[slot], s_wd.at[slot])

    def wgu_copy(k, j, slot):
        src = w_up if k else w_gate
        return pltpu.make_async_copy(src.at[pl.ds(j * ND, ND)], wgu.at[slot, k], s_wgu.at[slot, k])

    def gub_copies(p):
        b = block_of(p)
        out = []
        for k, src in enumerate((gate, up)):
            for i, core in enumerate((c, 1 - c)):
                rows = pl.ds((2 * b + core) * R, R)
                out.append(pltpu.make_async_copy(src.at[rows], gub.at[k, pl.ds(i * R, R)], s_gub.at[k, i]))
        return out

    def dyb_copy(i, src):
        return pltpu.make_async_copy(src, dyb.at[pl.ds(i * R, R)], s_dyb.at[i])

    def tile_copies(own, all_, i, slot):
        return rows_copies(own, all_, i, tile.at[slot], s_tile.at[slot], block_of, c)

    def keep(p):
        rows = pl.ds(pl.multiple_of(p * 2 * R, 2 * R), 2 * R)
        return [
            pltpu.make_async_copy(src.at[rows], dst.at[rows], s_keep.at[k, p])
            for k, (src, dst) in enumerate(((dg, dgo), (du, duo)))
        ]

    def start(copies):
        for cp in copies:
            cp.start()

    def wait(copies):
        for cp in copies:
            cp.wait()

    def half(k):
        return pl.ds(pl.multiple_of(k * K2, K2), K2)

    def pair_send(p, k):
        return remote(psend.at[p, :, half(k)], precv.at[p, :, half(k)], sp.at[p, k], rp.at[p, k], other)

    def run_recv(t, k):
        return remote(rrecv.at[t, :, half(k)], rrecv.at[t, :, half(k)], sr.at[0, k], rr.at[t, k], other)

    def run_send(p, k, to, t):
        return remote(rsend.at[p, :, half(k)], rrecv.at[t, :, half(k)], sr.at[p, k], rr.at[t, k], to)

    def add_terms(p, k, extra, out):
        loads = [
            pltpu.make_async_copy(pown.at[p, :, half(k)], rsf, s_rs.at[0]),
            pltpu.make_async_copy(precv.at[p, :, half(k)], rsb.at[0], s_rs.at[1]),
        ]
        for t in extra:
            loads.append(pltpu.make_async_copy(rrecv.at[t, :, half(k)], rsb.at[1], s_rs.at[2]))
        start(loads)
        wait(loads)
        wide = out.dtype == F32

        def body(i, _):
            rows = pl.ds(pl.multiple_of(i * 32, 32), 32)
            v = rsf[rows] + rsb[0, rows].astype(F32)
            if extra:
                v = v + rsb[1, rows].astype(F32)
            if wide:
                rsf[rows] = v
            else:
                rsb[2, rows] = v.astype(BF)
            return 0

        lax.fori_loop(0, R // 32, body, 0)
        cp = pltpu.make_async_copy(rsf if wide else rsb.at[2], out, s_rs.at[3])
        cp.start()
        cp.wait()

    def sum_up(p, k, mid, out):
        t = block_of(p)
        pair_send(p, k).wait_recv()
        if mid:
            run_recv(t, k).wait_recv()
        add_terms(p, k, (t,) if mid else (), out)
        return t

    def pass_on(p, k, mid):
        t = sum_up(p, k, mid, rsend.at[p, :, half(k)])

        @pl.when(t > z)
        def _():
            run_send(p, k, right, t).start()

        @pl.when(t < z)
        def _():
            run_send(p, k, left, jnp.where(t == z - 1, 4, t)).start()

    def halves(f):
        def body(k, _):
            f(k)
            return 0

        lax.fori_loop(0, 2, body, 0)

    barrier = pltpu.get_barrier_semaphore()

    def greet(to):
        pl.semaphore_signal(barrier, inc=1, device_id={"tp": to}, device_id_type=MESH)

    greet(other)

    @pl.when(z < 3)
    def _():
        greet(right)

    @pl.when(z > 0)
    def _():
        greet(left)

    for n in range(2):
        wd_copy(n, n).start()
    start(gub_copies(0))
    own_dyb = dyb_copy(0, dy)
    own_dyb.start()

    @pl.when(is_mid)
    def _():
        pl.semaphore_wait(barrier, 3)

    @pl.when(is_end)
    def _():
        pl.semaphore_wait(barrier, 2)

    for i in range(H):

        @pl.when(z < 3)
        def _():
            send_right(Dy, 0, i, Dy.own_at(i))

        @pl.when(z > 0)
        def _():
            send_left(Dy, 0, i, Dy.own_at(i))

        send_other(Dy, 0, 0, i, Dy.own_at(i))

    def end_x(i, _):
        @pl.when(z == 0)
        def _():
            send_right(X, 0, i, X.own_at(i))

        @pl.when(z == 3)
        def _():
            send_left(X, 0, i, X.own_at(i))

        return 0

    lax.fori_loop(0, Q, end_x, 0)
    for j in range(2):
        for k in range(2):
            wgu_copy(k, j, j).start()

    def phase(p, _):
        b = block_of(p)
        for i in range(H):
            wait_recv(Dy, 2 * b + 1 - c, i)
        theirs = dyb_copy(1, dyg.at[2 * b + 1 - c])
        theirs.start()

        @pl.when(p > 0)
        def _():
            dyb_copy(0, dyg.at[2 * b + c]).start()

        wait(gub_copies(p))
        own_dyb.wait()
        theirs.wait()
        rows = pl.ds(pl.multiple_of(p * 2 * R, 2 * R), 2 * R)

        def hidden_tile(n, _):
            slot = lax.rem(n, 2)
            cols = pl.ds(pl.multiple_of(n * NH, NH), NH)
            wd_copy(n, slot).wait()
            dh = dot(dyb[...], wd[slot], 1, 1)
            g = gub[0, :, cols].astype(F32)
            u = gub[1, :, cols].astype(F32)
            s = jax.nn.sigmoid(g)
            a = g * s
            hid[rows, cols] = (a * u).astype(BF)
            du[rows, cols] = (dh * a).astype(BF)
            dg[rows, cols] = (dh * (u * (s + a * (1.0 - s)))).astype(BF)

            @pl.when((n < F // NH - 2) | (p < 3))
            def _():
                wd_copy(lax.rem(n + 2, F // NH), slot).start()

            return 0

        lax.fori_loop(0, F // NH, hidden_tile, 0)

        start(keep(p))

        @pl.when(p < 3)
        def _():
            start(gub_copies(p + 1))

        @pl.when(p < 3)
        def _():
            hop(Dy, p + 1, 0)

        @pl.when(p >= 2)
        def _():
            x_step(2 * p - 3)

        def stage(j, slot):
            cols = pl.ds(pl.multiple_of(j * ND, ND), ND)
            return [
                pltpu.make_async_copy(stf.at[slot], pown.at[p, :, cols], s_st.at[0, slot]),
                pltpu.make_async_copy(stb.at[slot], psend.at[p, :, cols], s_st.at[1, slot]),
            ]

        def dx_tile(j, _):
            slot = lax.rem(j, 2)
            for k in range(2):
                wgu_copy(k, j, slot).wait()
            acc = dot(dg[rows, :], wgu[slot, 0], 1, 1) + dot(du[rows, :], wgu[slot, 1], 1, 1)

            @pl.when(j >= 2)
            def _():
                wait(stage(j - 2, slot))

            stf[slot] = acc[:R]
            stb[slot] = acc[R:].astype(BF)
            start(stage(j, slot))

            @pl.when((j < D // ND - 2) | (p < 3))
            def _():
                for k in range(2):
                    wgu_copy(k, lax.rem(j + 2, D // ND), slot).start()

            @pl.when(j == D // ND // 2 + 1)
            def _():
                pair_send(p, 0).start()

            return 0

        lax.fori_loop(0, D // ND, dx_tile, 0)
        for j in (D // ND - 2, D // ND - 1):
            wait(stage(j, j % 2))
        pair_send(p, 1).start()

        @pl.when(p < 3)
        def _():
            hop(Dy, p + 1, 1)

        @pl.when(p >= 1)
        def _():
            x_step(2 * p - 2)

            @pl.when(is_end)
            def _():
                halves(lambda k: pass_on(p, k, False))

        return 0

    lax.fori_loop(0, 4, phase, 0)

    def out_d(i, slot):
        cols = pl.ds(pl.multiple_of(i * ND, ND), ND)
        return pltpu.make_async_copy(ost.at[slot], dwd.at[:, cols], s_out.at[slot, 0])

    start(tile_copies(dy, dyg, 0, 0))

    def down_tile(i, _):
        slot = lax.rem(i, 2)

        @pl.when(i < D // ND - 1)
        def _():
            start(tile_copies(dy, dyg, i + 1, 1 - slot))

        @pl.when((i == 2) | (i == 4))
        def _():
            x_step(4 + i // 2)

        @pl.when(i == 7)
        def _():
            x_end(0)

        wait(tile_copies(dy, dyg, i, slot))

        @pl.when(i >= 2)
        def _():
            out_d(i - 2, slot).wait()

        for m in range(F // ND):
            ost[slot, m * ND : (m + 1) * ND, :] = dot(hid[:, m * ND : (m + 1) * ND], tile[slot], 0, 0).astype(BF)
        out_d(i, slot).start()
        return 0

    lax.fori_loop(0, D // ND, down_tile, 0)
    x_ready(0)
    start(tile_copies(x, xg, 0, 0))
    for i in (D // ND - 2, D // ND - 1):
        out_d(i, i % 2).wait()

    def out_gu(i, slot):
        rows = pl.ds(pl.multiple_of(i * ND, ND), ND)
        return [
            pltpu.make_async_copy(wgu.at[slot, k], (dwg, dwu)[k].at[rows], s_out.at[slot, k]) for k in range(2)
        ]

    def gu_tile(i, _):
        slot = lax.rem(i, 2)
        q = i // 2

        @pl.when((slot == 0) & (q < NF // 2 - 1))
        def _():
            x_end(q + 1)

        @pl.when((slot == 1) & (q < NF // 2 - 1))
        def _():
            x_ready(q + 1)

        @pl.when(i < NF - 1)
        def _():
            start(tile_copies(x, xg, i + 1, 1 - slot))

        @pl.when(is_mid & ((i == 0) | (i == 2)))
        def _():
            pass_on(3, i // 2, True)

        wait(tile_copies(x, xg, i, slot))

        @pl.when(i >= 2)
        def _():
            wait(out_gu(i - 2, slot))

        for k, r in enumerate((dg, du)):
            for n in range(2):
                wgu[slot, k, :, n * 1024 : (n + 1) * 1024] = dot(
                    tile[slot], r[:, n * 1024 : (n + 1) * 1024], 0, 0
                ).astype(BF)
        start(out_gu(i, slot))
        return 0

    lax.fori_loop(0, NF, gu_tile, 0)

    for i in range(NF // 2, Q):
        x_end(i)

    @pl.when(is_mid)
    def _():
        halves(lambda k: sum_up(1, k, True, s_end.at[:, half(k)]))
        halves(lambda k: sum_up(2, k, True, s_mid.at[:, half(k)]))

    def own_rows(k):
        pair_send(0, k).wait_recv()

        @pl.when(is_mid)
        def _():
            t = jnp.where(z == 1, 1, 4)
            run_recv(t, k).wait_recv()
            add_terms(0, k, (t,), dxa.at[:, half(k)])

        @pl.when(is_end)
        def _():
            add_terms(0, k, (), dxa.at[:, half(k)])

    halves(own_rows)
    for i in range(NF // 2, Q):
        x_ready(i)
    for p in range(4):
        wait(keep(p))
    for i in (NF - 2, NF - 1):
        wait(out_gu(i, i % 2))
    wait_sends(Dy)
    wait_sends(X)

    def sums(t, _):
        p, k = t // 2, lax.rem(t, 2)
        pair_send(p, k).wait_send()

        @pl.when((is_end & (p > 0)) | (is_mid & (p == 3)))
        def _():
            run_send(p, k, other, 0).wait_send()

        return 0

    lax.fori_loop(0, 8, sums, 0)


def rest(
    x, xg, dgi, dui, dwg_in, dwu_in, dwd_in, dwg, dwu, dwd,
    dg, du, tile, ost, bg, bd, s_in, s_tile, s_out, s_ci, s_co,
):
    me = lax.axis_index("tp")
    z = me // 2
    c = lax.rem(me, 2)

    def tile_copies(i, slot):
        return rows_copies(x, xg, i, tile.at[slot], s_tile.at[slot], lambda p: order(z, p), c)

    def moves(i, slot, out):
        rows = pl.ds(pl.multiple_of(i * ND, ND), ND)
        copies = []
        for k, (src, dst, buf) in enumerate(
            ((dwg_in, dwg, bg.at[slot, 0]), (dwu_in, dwu, bg.at[slot, 1]), (dwd_in, dwd, bd.at[slot]))
        ):
            if out:
                copies.append(pltpu.make_async_copy(buf, dst.at[rows], s_co.at[slot, k]))
            else:
                copies.append(pltpu.make_async_copy(src.at[rows], buf, s_ci.at[slot, k]))
        return copies

    def out_gu(i, slot):
        rows = pl.ds(pl.multiple_of(i * ND, ND), ND)
        return [
            pltpu.make_async_copy(ost.at[slot, k], (dwg, dwu)[k].at[rows], s_out.at[slot, k]) for k in range(2)
        ]

    def start(copies):
        for cp in copies:
            cp.start()

    def wait(copies):
        for cp in copies:
            cp.wait()

    whole = [pltpu.make_async_copy(s, d, s_in.at[k]) for k, (s, d) in enumerate(((dgi, dg), (dui, du)))]
    start(tile_copies(NF, 0))
    start(whole)

    def step(i, _):
        slot = lax.rem(i, 2)

        @pl.when(i < NT - NF - 1)
        def _():
            start(tile_copies(NF + i + 1, 1 - slot))

        wait(tile_copies(NF + i, slot))

        @pl.when(i >= 2)
        def _():
            wait(out_gu(NF + i - 2, slot))

        @pl.when((i >= 1) & (i < NF + 1))
        def _():
            wait(moves(i - 1, 1 - slot, False))
            start(moves(i - 1, 1 - slot, True))

        @pl.when((i >= 2) & (i < NF + 2))
        def _():
            wait(moves(i - 2, slot, True))

        @pl.when((i >= 2) & (i < NF))
        def _():
            start(moves(i, slot, False))

        for k, r in enumerate((dg, du)):

            @pl.when(i == 0)
            def _():
                whole[k].wait()
                if k:
                    start(moves(0, 0, False))
                    start(moves(1, 1, False))

            for n in range(2):
                ost[slot, k, :, n * 1024 : (n + 1) * 1024] = dot(
                    tile[slot], r[:, n * 1024 : (n + 1) * 1024], 0, 0
                ).astype(BF)
        start(out_gu(NF + i, slot))
        return 0

    lax.fori_loop(0, NT - NF, step, 0)
    for i in (NT - NF - 2, NT - NF - 1):
        wait(out_gu(NF + i, i % 2))


def finish(dxa, from_mid, across, dx, own, got, out, s_own, s_got, s_out):
    z = lax.axis_index("tp") // 2
    is_end = (z == 0) | (z == 3)
    n = R // 32

    def at(i):
        return pl.ds(pl.multiple_of(i * 32, 32), 32)

    def get(src, dst, sem, i):
        return pltpu.make_async_copy(src.at[at(i)], dst.at[at(i)], sem.at[i])

    def load(i, _):
        get(dxa, own, s_own, i).start()

        @pl.when(is_end)
        def _():
            get(from_mid, got, s_got, i).start()

        @pl.when(jnp.logical_not(is_end))
        def _():
            get(across, got, s_got, i).start()

        return 0

    def add(i, _):
        get(dxa, own, s_own, i).wait()
        get(from_mid, got, s_got, i).wait()
        out[at(i)] = (own[at(i)] + got[at(i)].astype(F32)).astype(BF)
        get(out, dx, s_out, i).start()
        return 0

    def end(i, _):
        get(out, dx, s_out, i).wait()
        return 0

    lax.fori_loop(0, n, load, 0)
    lax.fori_loop(0, n, add, 0)
    lax.fori_loop(0, n, end, 0)


def fused(x, dy, gate, up, w_gate, w_up, w_down):
    hbm = pl.BlockSpec(memory_space=pl.ANY)

    def arr(*shape, dtype=BF):
        return jax.ShapeDtypeStruct(shape, dtype)

    part = arr(NF * ND, F)
    outs = [
        arr(R, D, dtype=F32), part, part, arr(F, D), arr(8 * R, F), arr(8 * R, F), arr(8, R, D), arr(R, D), arr(R, D),
        arr(8, R, D), arr(4, R, D, dtype=F32), arr(4, R, D), arr(4, R, D), arr(4, R, D), arr(5, R, D),
    ]
    dma = pltpu.SemaphoreType.DMA
    scratch = [
        pltpu.VMEM((8 * R, F), BF), pltpu.VMEM((8 * R, F), BF), pltpu.VMEM((8 * R, F), BF),
        pltpu.VMEM((2 * R, D), BF), pltpu.VMEM((2, 2 * R, F), BF), pltpu.VMEM((2, NH, D), BF),
        pltpu.VMEM((2, 2, ND, F), BF), pltpu.VMEM((2, 8 * R, ND), BF), pltpu.VMEM((2, F, ND), BF),
        pltpu.VMEM((2, R, ND), F32), pltpu.VMEM((2, R, ND), BF), pltpu.VMEM((R, K2), F32),
        pltpu.VMEM((3, R, K2), BF),
        dma((2,)), dma((2, 2)), dma((2, 2)), dma((2,)), dma((2, 8)), dma((2, 2)), dma((2, 2)), dma((4,)), dma((2, 4)),
        dma((4, H)), dma((4, H)), dma((2, 4, H)), dma((8, H)),
        dma((4, Q)), dma((4, Q)), dma((2, 4, Q)), dma((8, Q)),
        dma((4, 2)), dma((4, 2)), dma((4, 2)), dma((5, 2)),
    ]
    made = pl.pallas_call(
        kernel,
        out_shape=outs,
        in_specs=[hbm] * 7,
        out_specs=[hbm] * len(outs),
        scratch_shapes=scratch,
        compiler_params=pltpu.CompilerParams(collective_id=0, has_side_effects=True, vmem_limit_bytes=67043328),
        cost_estimate=pl.CostEstimate(flops=180_000_000_000, bytes_accessed=500_000_000, transcendentals=4_000_000),
    )(x, dy, gate, up, w_gate, w_up, w_down)
    dxa, dwg, dwu, dwd, dgo, duo, xg, s_end, s_mid = made[:9]
    cores = range(2)
    from_mid = lax.ppermute(s_end, "tp", [(2 * a + k, 2 * b + k) for a, b in ((1, 0), (2, 3)) for k in cores])
    across = lax.ppermute(s_mid, "tp", [(2 * a + k, 2 * b + k) for a, b in ((1, 2), (2, 1)) for k in cores])
    full = [arr(D, F), arr(D, F), arr(F, D)]
    dwg, dwu, dwd = pl.pallas_call(
        rest,
        out_shape=full,
        in_specs=[hbm] * 7,
        out_specs=[hbm] * 3,
        scratch_shapes=[
            pltpu.VMEM((8 * R, F), BF), pltpu.VMEM((8 * R, F), BF), pltpu.VMEM((2, 8 * R, ND), BF),
            pltpu.VMEM((2, 2, ND, F), BF), pltpu.VMEM((2, 2, ND, F), BF), pltpu.VMEM((2, ND, D), BF),
            dma((2,)), dma((2, 8)), dma((2, 2)), dma((2, 3)), dma((2, 3)),
        ],
        compiler_params=pltpu.CompilerParams(vmem_limit_bytes=67043328),
        cost_estimate=pl.CostEstimate(flops=45_000_000_000, bytes_accessed=150_000_000, transcendentals=0),
    )(x, xg, dgo, duo, dwg, dwu, dwd)
    dx = pl.pallas_call(
        finish,
        out_shape=arr(R, D),
        in_specs=[hbm] * 3,
        out_specs=hbm,
        scratch_shapes=[
            pltpu.VMEM((R, D), F32), pltpu.VMEM((R, D), BF), pltpu.VMEM((R, D), BF), dma((7,)), dma((7,)), dma((7,)),
        ],
        compiler_params=pltpu.CompilerParams(vmem_limit_bytes=67043328),
        cost_estimate=pl.CostEstimate(flops=3_000_000, bytes_accessed=12_000_000, transcendentals=0),
    )(dxa, from_mid, across)
    return dx, dwg, dwu, dwd


def solution(mesh):
    rows, mine, cols = P(("dp", "tp"), None), P("dp", "tp"), P(None, "tp")
    return jax.shard_map(
        fused,
        mesh=mesh,
        in_specs=(rows, rows, mine, mine, cols, cols, P("tp", None)),
        out_specs=(rows, mine, mine, rows),
        check_vma=False,
    )
```

```python
import jax
import jax.numpy as jnp
from jax import lax
from jax.experimental import pallas as pl
from jax.experimental.pallas import tpu as pltpu
from jax.sharding import PartitionSpec as P

BF = jnp.bfloat16
F32 = jnp.float32
MESH = pl.DeviceIdType.MESH

R = 224
D = 5120
F = 2048
H = 2
HR = R // H
Q = 5
QC = D // Q
NH = 256
ND = 512
K2 = D // 2
RC = 32
NT = D // ND
NF = 4
NQ = (NF + 1) // 2
NM = 4


def dot(a, b, ca, cb):
    return lax.dot_general(a, b, (((ca,), (cb,)), ((), ())), preferred_element_type=F32)


def order(z, p):
    zz = jnp.where(z < 2, z, 3 - z)
    near = jnp.where((zz == 1) & (p < 2), 1 - p, p)
    return jnp.where(z < 2, near, 3 - near)


def rows_copies(own, all_, i, dst, sems, block_of, c):
    cols = pl.ds(i * ND, ND)
    out = []
    for p in range(4):
        b = block_of(p)
        for k, core in enumerate((c, 1 - c)):
            src = own.at[:, cols] if p == 0 and k == 0 else all_.at[2 * b + core, :, cols]
            out.append(pltpu.make_async_copy(src, dst.at[pl.ds((2 * p + k) * R, R)], sems.at[2 * p + k]))
    return out


def kernel(
    x, dy, gate, up, w_gate, w_up, w_down,
    dxa, dwg, dwu, dwd, dgo, duo, xg, s_end, s_mid, dyg, pown, psend, precv, rsend, rrecv,
    hid, dg, du, dyb, gub, wd, wgu, tile, ost, stf, stb, rsf, rsb,
    s_wd, s_wgu, s_gub, s_dyb, s_tile, s_out, s_st, s_rs, s_keep,
    sd_r, sd_l, sd_p, rd, sx_r, sx_l, sx_p, rx, sp, rp, sr, rr,
):
    me = lax.axis_index("tp")
    z = me // 2
    c = lax.rem(me, 2)
    other = me + 1 - 2 * c
    right, left = me + 2, me - 2
    is_end = (z == 0) | (z == 3)
    is_mid = (z == 1) | (z == 2)

    def block_of(p):
        return order(z, p)

    def remote(src, dst, ssem, rsem, to):
        return pltpu.make_async_remote_copy(
            src_ref=src, dst_ref=dst, send_sem=ssem, recv_sem=rsem, device_id={"tp": to}, device_id_type=MESH
        )

    class Dy:
        own, all_, rs, ls, ps, rv, n = dy, dyg, sd_r, sd_l, sd_p, rd, H

        @staticmethod
        def own_at(i):
            return dy.at[pl.ds(i * HR, HR)]

        @staticmethod
        def at(blk, i):
            return dyg.at[blk, pl.ds(i * HR, HR)]

    class X:
        own, all_, rs, ls, ps, rv, n = x, xg, sx_r, sx_l, sx_p, rx, Q

        @staticmethod
        def own_at(i):
            return x.at[:, pl.ds(i * QC, QC)]

        @staticmethod
        def at(blk, i):
            return xg.at[blk, :, pl.ds(i * QC, QC)]

    def send_right(g, d, i, src):
        blk = me - 2 * d
        remote(src, g.at(blk, i), g.rs.at[d, i], g.rv.at[blk, i], right).start()

    def send_left(g, d, i, src):
        blk = me + 2 * d
        remote(src, g.at(blk, i), g.ls.at[d, i], g.rv.at[blk, i], left).start()

    def send_other(g, side, d, i, src):
        blk = me + (2 * d if side else -2 * d)
        remote(src, g.at(blk, i), g.ps.at[side, d, i], g.rv.at[blk, i], other).start()

    def wait_recv(g, blk, i):
        remote(g.at(blk, i), g.at(blk, i), g.ps.at[0, 0, i], g.rv.at[blk, i], other).wait_recv()

    def hop(g, d, i, gate_=True):
        @pl.when((z >= d) & gate_)
        def _():
            blk = me - 2 * d
            wait_recv(g, blk, i)

            @pl.when(z < 3)
            def _():
                send_right(g, d, i, g.at(blk, i))

            send_other(g, 0, d, i, g.at(blk, i))

        @pl.when((z + d <= 3) & gate_)
        def _():
            blk = me + 2 * d
            wait_recv(g, blk, i)

            @pl.when(z > 0)
            def _():
                send_left(g, d, i, g.at(blk, i))

            send_other(g, 1, d, i, g.at(blk, i))

    def wait_sends(g):
        def body(t, _):
            d, i = t // g.n, lax.rem(t, g.n)

            @pl.when((z < 3) & (d <= z))
            def _():
                remote(g.at(me, i), g.at(me, i), g.rs.at[d, i], g.rv.at[me, i], other).wait_send()

            @pl.when((z > 0) & (d <= 3 - z))
            def _():
                remote(g.at(me, i), g.at(me, i), g.ls.at[d, i], g.rv.at[me, i], other).wait_send()

            @pl.when(d <= z)
            def _():
                remote(g.at(me, i), g.at(me, i), g.ps.at[0, d, i], g.rv.at[me, i], other).wait_send()

            @pl.when((d > 0) & (d <= 3 - z))
            def _():
                remote(g.at(me, i), g.at(me, i), g.ps.at[1, d, i], g.rv.at[me, i], other).wait_send()

            return 0

        lax.fori_loop(0, 4 * g.n, body, 0)

    def x_step(s):
        @pl.when(s < Q)
        def _():
            send_other(X, 0, 0, s, X.own_at(s))

            @pl.when(is_mid)
            def _():
                send_right(X, 0, s, X.own_at(s))
                send_left(X, 0, s, X.own_at(s))

        @pl.when((s >= 1) & (s < Q + 1))
        def _():
            hop(X, 1, s - 1, is_mid)

        @pl.when((s >= 2) & (s < Q + 2))
        def _():
            hop(X, 2, s - 2, is_mid)

    def x_end(i):
        for d in (1, 2, 3):
            hop(X, d, i, is_end)

    def x_ready(i):
        for b in range(4):
            wait_recv(X, 2 * b + 1 - c, i)

    def wd_copy(n, slot):
        return pltpu.make_async_copy(w_down.at[pl.ds(n * NH, NH)], wd.at[slot], s_wd.at[slot])

    def wgu_copy(k, j, slot):
        src = w_up if k else w_gate
        return pltpu.make_async_copy(src.at[pl.ds(j * ND, ND)], wgu.at[slot, k], s_wgu.at[slot, k])

    def gub_copies(p):
        b = block_of(p)
        out = []
        for k, src in enumerate((gate, up)):
            for i, core in enumerate((c, 1 - c)):
                rows = pl.ds((2 * b + core) * R, R)
                out.append(pltpu.make_async_copy(src.at[rows], gub.at[k, pl.ds(i * R, R)], s_gub.at[k, i]))
        return out

    def dyb_copy(i, src):
        return pltpu.make_async_copy(src, dyb.at[pl.ds(i * R, R)], s_dyb.at[i])

    def tile_copies(own, all_, i, slot):
        return rows_copies(own, all_, i, tile.at[slot], s_tile.at[slot], block_of, c)

    def keep(p):
        rows = pl.ds(pl.multiple_of(p * 2 * R, 2 * R), 2 * R)
        return [
            pltpu.make_async_copy(src.at[rows], dst.at[rows], s_keep.at[k, p])
            for k, (src, dst) in enumerate(((dg, dgo), (du, duo)))
        ]

    def start(copies):
        for cp in copies:
            cp.start()

    def wait(copies):
        for cp in copies:
            cp.wait()

    def half(k):
        return pl.ds(pl.multiple_of(k * K2, K2), K2)

    def pair_send(p, k):
        return remote(psend.at[p, :, half(k)], precv.at[p, :, half(k)], sp.at[p, k], rp.at[p, k], other)

    def run_recv(t, k):
        return remote(rrecv.at[t, :, half(k)], rrecv.at[t, :, half(k)], sr.at[0, k], rr.at[t, k], other)

    def run_send(p, k, to, t):
        return remote(rsend.at[p, :, half(k)], rrecv.at[t, :, half(k)], sr.at[p, k], rr.at[t, k], to)

    def add_terms(p, k, extra, out):
        wide = out.dtype == F32
        srcs = [(pown.at[p], rsf), (precv.at[p], rsb.at[0])] + [(rrecv.at[t], rsb.at[1]) for t in extra]
        res = rsf if wide else rsb.at[2]

        def at(i):
            return pl.ds(pl.multiple_of(i * RC, RC), RC)

        def loads(i):
            return [
                pltpu.make_async_copy(src.at[at(i), half(k)], dst.at[at(i)], s_rs.at[n, i])
                for n, (src, dst) in enumerate(srcs)
            ]

        def store(i):
            return pltpu.make_async_copy(res.at[at(i)], out.at[at(i), half(k)], s_rs.at[3, i])

        def first(i, _):
            start(loads(i))
            return 0

        def body(i, _):
            wait(loads(i))
            rows = at(i)
            v = rsf[rows] + rsb[0, rows].astype(F32)
            if extra:
                v = v + rsb[1, rows].astype(F32)
            if wide:
                rsf[rows] = v
            else:
                rsb[2, rows] = v.astype(BF)
            store(i).start()
            return 0

        def final(i, _):
            store(i).wait()
            return 0

        for f in (first, body, final):
            lax.fori_loop(0, R // RC, f, 0)

    def sum_up(p, k, mid, out):
        t = block_of(p)
        pair_send(p, k).wait_recv()
        if mid:
            run_recv(t, k).wait_recv()
        add_terms(p, k, (t,) if mid else (), out)
        return t

    def pass_on(p, k, mid):
        t = sum_up(p, k, mid, rsend.at[p])

        @pl.when(t > z)
        def _():
            run_send(p, k, right, t).start()

        @pl.when(t < z)
        def _():
            run_send(p, k, left, jnp.where(t == z - 1, 4, t)).start()

    def halves(f):
        def body(k, _):
            f(k)
            return 0

        lax.fori_loop(0, 2, body, 0)

    barrier = pltpu.get_barrier_semaphore()

    def greet(to):
        pl.semaphore_signal(barrier, inc=1, device_id={"tp": to}, device_id_type=MESH)

    greet(other)

    @pl.when(z < 3)
    def _():
        greet(right)

    @pl.when(z > 0)
    def _():
        greet(left)

    for n in range(2):
        wd_copy(n, n).start()
    start(gub_copies(0))
    own_dyb = dyb_copy(0, dy)
    own_dyb.start()

    @pl.when(is_mid)
    def _():
        pl.semaphore_wait(barrier, 3)

    @pl.when(is_end)
    def _():
        pl.semaphore_wait(barrier, 2)

    for i in range(H):

        @pl.when(z < 3)
        def _():
            send_right(Dy, 0, i, Dy.own_at(i))

        @pl.when(z > 0)
        def _():
            send_left(Dy, 0, i, Dy.own_at(i))

        send_other(Dy, 0, 0, i, Dy.own_at(i))

    def end_x(i, _):
        @pl.when(z == 0)
        def _():
            send_right(X, 0, i, X.own_at(i))

        @pl.when(z == 3)
        def _():
            send_left(X, 0, i, X.own_at(i))

        return 0

    lax.fori_loop(0, Q, end_x, 0)
    for j in range(2):
        for k in range(2):
            wgu_copy(k, j, j).start()

    def phase(p, _):
        b = block_of(p)
        for i in range(H):
            wait_recv(Dy, 2 * b + 1 - c, i)
        theirs = dyb_copy(1, dyg.at[2 * b + 1 - c])
        theirs.start()

        @pl.when(p > 0)
        def _():
            dyb_copy(0, dyg.at[2 * b + c]).start()

        wait(gub_copies(p))
        own_dyb.wait()
        theirs.wait()
        rows = pl.ds(pl.multiple_of(p * 2 * R, 2 * R), 2 * R)

        def hidden_tile(n, _):
            slot = lax.rem(n, 2)
            cols = pl.ds(pl.multiple_of(n * NH, NH), NH)
            wd_copy(n, slot).wait()
            dh = dot(dyb[...], wd[slot], 1, 1)
            g = gub[0, :, cols].astype(F32)
            u = gub[1, :, cols].astype(F32)
            s = jax.nn.sigmoid(g)
            a = g * s
            hid[rows, cols] = (a * u).astype(BF)
            du[rows, cols] = (dh * a).astype(BF)
            dg[rows, cols] = (dh * (u * (s + a * (1.0 - s)))).astype(BF)

            @pl.when((n < F // NH - 2) | (p < 3))
            def _():
                wd_copy(lax.rem(n + 2, F // NH), slot).start()

            return 0

        lax.fori_loop(0, F // NH, hidden_tile, 0)

        start(keep(p))

        @pl.when(p < 3)
        def _():
            start(gub_copies(p + 1))

        @pl.when(p < 3)
        def _():
            hop(Dy, p + 1, 0)

        @pl.when(p >= 2)
        def _():
            x_step(2 * p - 3)

        def stage(j, slot):
            cols = pl.ds(pl.multiple_of(j * ND, ND), ND)
            return [
                pltpu.make_async_copy(stf.at[slot], pown.at[p, :, cols], s_st.at[0, slot]),
                pltpu.make_async_copy(stb.at[slot], psend.at[p, :, cols], s_st.at[1, slot]),
            ]

        def dx_tile(j, _):
            slot = lax.rem(j, 2)
            for k in range(2):
                wgu_copy(k, j, slot).wait()
            acc = dot(dg[rows, :], wgu[slot, 0], 1, 1) + dot(du[rows, :], wgu[slot, 1], 1, 1)

            @pl.when(j >= 2)
            def _():
                wait(stage(j - 2, slot))

            stf[slot] = acc[:R]
            stb[slot] = acc[R:].astype(BF)
            start(stage(j, slot))

            @pl.when((j < D // ND - 2) | (p < 3))
            def _():
                for k in range(2):
                    wgu_copy(k, lax.rem(j + 2, D // ND), slot).start()

            @pl.when(j == D // ND // 2 + 1)
            def _():
                pair_send(p, 0).start()

            return 0

        lax.fori_loop(0, D // ND, dx_tile, 0)
        for j in (D // ND - 2, D // ND - 1):
            wait(stage(j, j % 2))
        pair_send(p, 1).start()

        @pl.when(p < 3)
        def _():
            hop(Dy, p + 1, 1)

        @pl.when(p >= 1)
        def _():
            x_step(2 * p - 2)

            @pl.when(is_end)
            def _():
                halves(lambda k: pass_on(p, k, False))

        return 0

    lax.fori_loop(0, 4, phase, 0)

    def out_d(i, slot):
        cols = pl.ds(pl.multiple_of(i * ND, ND), ND)
        return pltpu.make_async_copy(ost.at[slot], dwd.at[:, cols], s_out.at[slot, 0])

    start(tile_copies(dy, dyg, 0, 0))

    def down_tile(i, _):
        slot = lax.rem(i, 2)

        @pl.when(i < D // ND - 1)
        def _():
            start(tile_copies(dy, dyg, i + 1, 1 - slot))

        @pl.when((i == 2) | (i == 4))
        def _():
            x_step(4 + i // 2)

        @pl.when(i == 7)
        def _():
            x_end(0)

        wait(tile_copies(dy, dyg, i, slot))

        @pl.when(i >= 2)
        def _():
            out_d(i - 2, slot).wait()

        for m in range(F // ND):
            ost[slot, m * ND : (m + 1) * ND, :] = dot(hid[:, m * ND : (m + 1) * ND], tile[slot], 0, 0).astype(BF)
        out_d(i, slot).start()
        return 0

    lax.fori_loop(0, D // ND, down_tile, 0)
    x_ready(0)
    start(tile_copies(x, xg, 0, 0))
    for i in (D // ND - 2, D // ND - 1):
        out_d(i, i % 2).wait()

    def out_gu(i, slot):
        rows = pl.ds(pl.multiple_of(i * ND, ND), ND)
        return [
            pltpu.make_async_copy(wgu.at[slot, k], (dwg, dwu)[k].at[rows], s_out.at[slot, k]) for k in range(2)
        ]

    def gu_tile(i, _):
        slot = lax.rem(i, 2)
        q = i // 2

        @pl.when((slot == 0) & (q < NQ - 1))
        def _():
            x_end(q + 1)

        @pl.when((slot == 1) & (q < NQ - 1))
        def _():
            x_ready(q + 1)

        @pl.when(i < NF - 1)
        def _():
            start(tile_copies(x, xg, i + 1, 1 - slot))

        @pl.when(is_mid & ((i == 1) | (i == NF - 1)))
        def _():
            pass_on(3, i // (NF - 1), True)

        wait(tile_copies(x, xg, i, slot))

        @pl.when(i >= 2)
        def _():
            wait(out_gu(i - 2, slot))

        for k, r in enumerate((dg, du)):
            for n in range(2):
                wgu[slot, k, :, n * 1024 : (n + 1) * 1024] = dot(
                    tile[slot], r[:, n * 1024 : (n + 1) * 1024], 0, 0
                ).astype(BF)
        start(out_gu(i, slot))
        return 0

    lax.fori_loop(0, NF, gu_tile, 0)

    for i in range(NQ, Q):
        x_end(i)

    @pl.when(is_mid)
    def _():
        sum_up(1, 0, True, s_end)
        halves(lambda k: sum_up(2, k, True, s_mid))

    def own_rows(k):
        pair_send(0, k).wait_recv()

        @pl.when(is_mid)
        def _():
            t = jnp.where(z == 1, 1, 4)
            run_recv(t, k).wait_recv()
            add_terms(0, k, (t,), dxa)

        @pl.when(is_end)
        def _():
            add_terms(0, k, (), dxa)

    halves(own_rows)

    @pl.when(is_mid)
    def _():
        sum_up(1, 1, True, s_end)

    for i in range(NQ, Q):
        x_ready(i)
    for p in range(4):
        wait(keep(p))
    for i in (NF - 2, NF - 1):
        wait(out_gu(i, i % 2))
    wait_sends(Dy)
    wait_sends(X)

    def sums(t, _):
        p, k = t // 2, lax.rem(t, 2)
        pair_send(p, k).wait_send()

        @pl.when((is_end & (p > 0)) | (is_mid & (p == 3)))
        def _():
            run_send(p, k, other, 0).wait_send()

        return 0

    lax.fori_loop(0, 8, sums, 0)


def rest(
    x, xg, dgi, dui, dwg_in, dwu_in, dwd_in, dwg, dwu, dwd,
    dg, du, tile, ost, bg, bd, s_in, s_tile, s_out, s_ci, s_co,
):
    me = lax.axis_index("tp")
    z = me // 2
    c = lax.rem(me, 2)

    def tile_copies(i, slot):
        return rows_copies(x, xg, i, tile.at[slot], s_tile.at[slot], lambda p: order(z, p), c)

    def moves(i, slot, out):
        copies = []
        for k, (src, dst, buf) in enumerate(
            ((dwg_in, dwg, bg.at[slot, 0]), (dwu_in, dwu, bg.at[slot, 1]), (dwd_in, dwd, bd.at[slot]))
        ):
            n = buf.shape[0]
            rows = pl.ds(pl.multiple_of(i * n, n), n)
            if out:
                copies.append(pltpu.make_async_copy(buf, dst.at[rows], s_co.at[slot, k]))
            else:
                copies.append(pltpu.make_async_copy(src.at[rows], buf, s_ci.at[slot, k]))
        return copies

    def out_gu(i, slot):
        rows = pl.ds(pl.multiple_of(i * ND, ND), ND)
        return [
            pltpu.make_async_copy(ost.at[slot, k], (dwg, dwu)[k].at[rows], s_out.at[slot, k]) for k in range(2)
        ]

    def start(copies):
        for cp in copies:
            cp.start()

    def wait(copies):
        for cp in copies:
            cp.wait()

    def whole(k, n):
        cols = pl.ds(n * 1024, 1024)
        return pltpu.make_async_copy((dgi, dui)[k].at[:, cols], (dg, du)[k].at[:, cols], s_in.at[k, n])

    start(tile_copies(NF, 0))
    for k in range(2):
        for n in range(2):
            whole(k, n).start()

    def step(i, _):
        slot = lax.rem(i, 2)

        @pl.when(i < NT - NF - 1)
        def _():
            start(tile_copies(NF + i + 1, 1 - slot))

        wait(tile_copies(NF + i, slot))

        @pl.when(i >= 2)
        def _():
            wait(out_gu(NF + i - 2, slot))

        @pl.when((i >= 1) & (i < NM + 1))
        def _():
            wait(moves(i - 1, 1 - slot, False))
            start(moves(i - 1, 1 - slot, True))

        @pl.when((i >= 2) & (i < NM + 2))
        def _():
            wait(moves(i - 2, slot, True))

        @pl.when((i >= 2) & (i < NM))
        def _():
            start(moves(i, slot, False))

        for k, r in enumerate((dg, du)):
            for n in range(2):

                @pl.when(i == 0)
                def _():
                    whole(k, n).wait()
                    if k and n:
                        start(moves(0, 0, False))
                        start(moves(1, 1, False))

                ost[slot, k, :, n * 1024 : (n + 1) * 1024] = dot(
                    tile[slot], r[:, n * 1024 : (n + 1) * 1024], 0, 0
                ).astype(BF)
        start(out_gu(NF + i, slot))
        return 0

    lax.fori_loop(0, NT - NF, step, 0)
    if NT - NF == NM:
        wait(moves(NM - 1, (NM - 1) % 2, False))
        start(moves(NM - 1, (NM - 1) % 2, True))
    for i in (NM - 2, NM - 1):
        if i + 2 > NT - NF - 1:
            wait(moves(i, i % 2, True))
    for i in (NT - NF - 2, NT - NF - 1):
        wait(out_gu(NF + i, i % 2))


def finish(dxa, from_mid, across, dx, own, got, out, s_own, s_got, s_out):
    z = lax.axis_index("tp") // 2
    is_end = (z == 0) | (z == 3)
    n = R // 32

    def at(i):
        return pl.ds(pl.multiple_of(i * 32, 32), 32)

    def get(src, dst, sem, i):
        return pltpu.make_async_copy(src.at[at(i)], dst.at[at(i)], sem.at[i])

    def load(i, _):
        get(dxa, own, s_own, i).start()

        @pl.when(is_end)
        def _():
            get(from_mid, got, s_got, i).start()

        @pl.when(jnp.logical_not(is_end))
        def _():
            get(across, got, s_got, i).start()

        return 0

    def add(i, _):
        get(dxa, own, s_own, i).wait()
        get(from_mid, got, s_got, i).wait()
        out[at(i)] = (own[at(i)] + got[at(i)].astype(F32)).astype(BF)
        get(out, dx, s_out, i).start()
        return 0

    def end(i, _):
        get(out, dx, s_out, i).wait()
        return 0

    lax.fori_loop(0, n, load, 0)
    lax.fori_loop(0, n, add, 0)
    lax.fori_loop(0, n, end, 0)


def fused(x, dy, gate, up, w_gate, w_up, w_down):
    hbm = pl.BlockSpec(memory_space=pl.ANY)

    def arr(*shape, dtype=BF):
        return jax.ShapeDtypeStruct(shape, dtype)

    part = arr(NF * ND, F)
    outs = [
        arr(R, D, dtype=F32), part, part, arr(F, D), arr(8 * R, F), arr(8 * R, F), arr(8, R, D), arr(R, D), arr(R, D),
        arr(8, R, D), arr(4, R, D, dtype=F32), arr(4, R, D), arr(4, R, D), arr(4, R, D), arr(5, R, D),
    ]
    dma = pltpu.SemaphoreType.DMA
    scratch = [
        pltpu.VMEM((8 * R, F), BF), pltpu.VMEM((8 * R, F), BF), pltpu.VMEM((8 * R, F), BF),
        pltpu.VMEM((2 * R, D), BF), pltpu.VMEM((2, 2 * R, F), BF), pltpu.VMEM((2, NH, D), BF),
        pltpu.VMEM((2, 2, ND, F), BF), pltpu.VMEM((2, 8 * R, ND), BF), pltpu.VMEM((2, F, ND), BF),
        pltpu.VMEM((2, R, ND), F32), pltpu.VMEM((2, R, ND), BF), pltpu.VMEM((R, K2), F32),
        pltpu.VMEM((3, R, K2), BF),
        dma((2,)), dma((2, 2)), dma((2, 2)), dma((2,)), dma((2, 8)), dma((2, 2)), dma((2, 2)), dma((4, R // RC)), dma((2, 4)),
        dma((4, H)), dma((4, H)), dma((2, 4, H)), dma((8, H)),
        dma((4, Q)), dma((4, Q)), dma((2, 4, Q)), dma((8, Q)),
        dma((4, 2)), dma((4, 2)), dma((4, 2)), dma((5, 2)),
    ]
    made = pl.pallas_call(
        kernel,
        out_shape=outs,
        in_specs=[hbm] * 7,
        out_specs=[hbm] * len(outs),
        scratch_shapes=scratch,
        compiler_params=pltpu.CompilerParams(collective_id=0, has_side_effects=True, vmem_limit_bytes=67043328),
        cost_estimate=pl.CostEstimate(flops=180_000_000_000, bytes_accessed=500_000_000, transcendentals=4_000_000),
    )(x, dy, gate, up, w_gate, w_up, w_down)
    dxa, dwg, dwu, dwd, dgo, duo, xg, s_end, s_mid = made[:9]
    cores = range(2)
    from_mid = lax.ppermute(s_end, "tp", [(2 * a + k, 2 * b + k) for a, b in ((1, 0), (2, 3)) for k in cores])
    across = lax.ppermute(s_mid, "tp", [(2 * a + k, 2 * b + k) for a, b in ((1, 2), (2, 1)) for k in cores])
    full = [arr(D, F), arr(D, F), arr(F, D)]
    dwg, dwu, dwd = pl.pallas_call(
        rest,
        out_shape=full,
        in_specs=[hbm] * 7,
        out_specs=[hbm] * 3,
        scratch_shapes=[
            pltpu.VMEM((8 * R, F), BF), pltpu.VMEM((8 * R, F), BF), pltpu.VMEM((2, 8 * R, ND), BF),
            pltpu.VMEM((2, 2, ND, F), BF), pltpu.VMEM((2, 2, NF * ND // NM, F), BF), pltpu.VMEM((2, F // NM, D), BF),
            dma((2, 2)), dma((2, 8)), dma((2, 2)), dma((2, 3)), dma((2, 3)),
        ],
        compiler_params=pltpu.CompilerParams(vmem_limit_bytes=67043328),
        cost_estimate=pl.CostEstimate(flops=45_000_000_000, bytes_accessed=150_000_000, transcendentals=0),
    )(x, xg, dgo, duo, dwg, dwu, dwd)
    dx = pl.pallas_call(
        finish,
        out_shape=arr(R, D),
        in_specs=[hbm] * 3,
        out_specs=hbm,
        scratch_shapes=[
            pltpu.VMEM((R, D), F32), pltpu.VMEM((R, D), BF), pltpu.VMEM((R, D), BF), dma((7,)), dma((7,)), dma((7,)),
        ],
        compiler_params=pltpu.CompilerParams(vmem_limit_bytes=67043328),
        cost_estimate=pl.CostEstimate(flops=3_000_000, bytes_accessed=12_000_000, transcendentals=0),
    )(dxa, from_mid, across)
    return dx, dwg, dwu, dwd


def solution(mesh):
    rows, mine, cols = P(("dp", "tp"), None), P("dp", "tp"), P(None, "tp")
    return jax.shard_map(
        fused,
        mesh=mesh,
        in_specs=(rows, rows, mine, mine, cols, cols, P("tp", None)),
        out_specs=(rows, mine, mine, rows),
        check_vma=False,
    )
```
